32 devices in a mesh: parts: 2 (over y), tok: 4 (over z), hid: 4 (over x, core).
Axes of the slice: x: 2, y: 2, z: 4, core: 2. Of those that a mesh axis runs over, the one named last changes fastest.
Arguments:
- tokens: bfloat16 [6144, 8192], P(('parts', 'tok'), 'hid'), parts along dimension 0, may hold values from -6 to 6
- adapter_ids: int32 [6144, 1], P(('parts', 'tok')), parts along dimension 0, may hold values from 0 to 31; in each aligned block of 768 rows (0 to 767, 768 to 1535, ...) at most 72 rows name the same one
- value_weight: bfloat16 [8192, 1024], P('hid'), may hold values from -0.0625 to 0.0625
- adapter_down: bfloat16 [32, 16, 8192], P('tok', None, 'hid'), may hold values from -0.0625 to 0.0625
- adapter_up: bfloat16 [32, 16, 1024], P('tok', None, 'hid'), may hold values from -1.5 to 1.5
Outputs:
- value_out: bfloat16 [6144, 1024], P(('parts', 'tok'), 'hid'), parts along dimension 0
The draws below stay inside these ranges and needn't reach their ends.
There are 2 independent parts, one for each index of `parts`. The reference program is written for one: setup_inputs(seed, part) draws one part's arguments, and reference() takes and returns one part's arrays. A program takes and returns all parts, laid end to end along the dimension named above; an argument that names none is the same for every part. Nothing has to cross between parts.
Inputs may be any that keep to these rules, and one draw needn't show every extreme that they name: `adapter_ids`: among the 768 tokens of one index of tok, each adapter id appears at most 72 times; in some of these aligned blocks one id appears exactly 72 times.
All inputs are finite; a program needn't handle non-finite values.
Results may differ from the reference program's by a relative error of at most 0.0048.
Values may be sent and summed in bfloat16 or wider, within the bound.
A program may use at most 128 MiB of HBM per device.

```python
import math
import jax
import jax.numpy as jnp
import numpy as np
from jax import lax

D = 8192
KV = 1024
R = 16
TOK_DEV = 768
ADAPTERS = 32
CAP = 72
TOKENS = 3072


def levels(own_key, dims, shards, smallest, high):
    gain, own = 1.0, jax.random.fold_in(own_key, 6)
    for position, shards_of in shards:
        steps = jnp.exp(jax.random.uniform(jax.random.fold_in(own, position), (shards_of,), jnp.float32, smallest / len(shards), high / len(shards)))
        gain = gain * jnp.repeat(steps, dims[position] // shards_of).reshape([-1 if axis == position else 1 for axis in range(len(dims))])
    return gain


def routed_block(key, own, number, rows, number_of, top, reach, lean):
    ranking = jax.random.permutation(key, number_of)
    heavy_load, common = portions_of(number_of, rows * top, reach, lean, True), portions_of(number_of, rows * top, reach, lean, False)
    places = jnp.arange(number_of)

    def named(tallies, offset_by):
        used = int((tallies > 0).sum())
        fixed = max(1, used // 4)
        moved = fixed + (places - fixed + offset_by * (used - fixed)) % max(1, number_of - fixed)
        return jnp.zeros((number_of,), jnp.int32).at[ranking[jnp.where(places < fixed, places, moved)]].set(jnp.asarray(tallies, jnp.int32))

    tallies = jnp.where(number % 4 == 0, named(heavy_load, number // 4), named(common, number - number // 4 - 1))
    mixed = jax.random.permutation(jax.random.fold_in(own, 3), number_of)
    source_of, receiver = mixed[0:number_of // 2 * 2:2], mixed[1:number_of // 2 * 2:2]
    slack = jnp.minimum(tallies[source_of] - 1, reach - tallies[receiver]) // 2
    slack = jnp.where((source_of == ranking[0]) | (receiver == ranking[0]) | (tallies[receiver] == 0), 0, jnp.maximum(slack, 0))
    moved = jax.random.randint(jax.random.fold_in(own, 4), (number_of // 2,), 0, 1 << 20) % (slack + 1)
    tallies = tallies.at[source_of].add(-moved).at[receiver].add(moved)
    labels = jnp.searchsorted(jnp.cumsum(tallies), jnp.arange(rows * top), side="right").astype(jnp.int32)
    listing = labels.reshape(top, rows).T
    listing = listing[jax.random.permutation(jax.random.fold_in(own, 1), rows)]
    offset_by = jax.random.randint(jax.random.fold_in(own, 2), (rows, 1), 0, top)
    return jnp.take_along_axis(listing, (jnp.arange(top)[None, :] + offset_by) % top, axis=1)


def portions_of(number_of, total, limit, slope, full):
    portions = [(1 << 20) // math.isqrt(grade ** slope) + 1 for grade in range(1, number_of + 1)]
    largest = limit if full else min(limit, max(-(-total // number_of), total * portions[0] // sum(portions)))
    least = 1 if total - largest >= number_of - 1 else 0
    holding, spare = [largest] + [least] * (number_of - 1), total - largest - least * (number_of - 1)
    while spare > 0:
        candidates = [i for i in range(1, number_of) if holding[i] < largest] or [i for i in range(1, number_of) if holding[i] < limit]
        mass, remaining = sum([portions[i] for i in candidates]), spare
        for i in candidates:
            extra = min(limit - holding[i], max(1, remaining * portions[i] // mass), spare)
            holding[i] = holding[i] + extra
            spare = spare - extra
    return np.array(holding)


def noise(key, extent, scale, most, cuts=(), held_as=jnp.bfloat16):
    result = scale * jax.random.normal(key, extent, jnp.float32)
    if cuts:
        result = result * levels(key, extent, cuts, -0.22, 0.18)
    return jnp.clip(result, -most, most).astype(held_as)


def setup_inputs(seed: int = 0, part: int = 0) -> dict:
    seeds = jax.random.split(jax.random.key(seed), 6)
    part_keys = jax.random.split(jax.random.fold_in(seeds[5], part), 6)
    tokens = noise(part_keys[0], (TOKENS, D), 1.0, 6.0, ((0, 4), (1, 4)))
    adapter_ids_keys = jax.random.split(jax.random.fold_in(part_keys[1], 1), TOKENS // TOK_DEV)
    adapter_ids_turns = jax.random.permutation(jax.random.fold_in(part_keys[1], 3), TOKENS // TOK_DEV)
    adapter_ids = jax.vmap(lambda own, number: routed_block(jax.random.fold_in(part_keys[1], 2), own, number, TOK_DEV, ADAPTERS, 1, CAP, 2))(adapter_ids_keys, adapter_ids_turns).reshape((TOKENS, 1))
    value_weight = noise(seeds[2], (D, KV), D ** -0.5, 0.0625, ((0, 4),))
    adapter_down = noise(seeds[3], (ADAPTERS, R, D), D ** -0.5, 0.0625, ((0, 4), (2, 4)))
    adapter_up = noise(seeds[4], (ADAPTERS, R, KV), R ** -0.5, 1.5, ((0, 4), (2, 4)))
    return {"tokens": tokens, "adapter_ids": adapter_ids, "value_weight": value_weight, "adapter_down": adapter_down, "adapter_up": adapter_up}


def reference(tokens, adapter_ids, value_weight, adapter_down, adapter_up):
    base_sums = jnp.dot(tokens, value_weight, preferred_element_type=jnp.float32)
    block_rows = math.gcd(TOKENS, 512)
    block_count = TOKENS // block_rows
    token_blocks = tokens.reshape(block_count, block_rows, D)
    id_blocks = adapter_ids[:, 0].reshape(block_count, block_rows)

    def block_delta(block_args):
        rows_block, ids_block = block_args
        down_picked = adapter_down[ids_block].astype(jnp.float32)
        low_rows = jnp.einsum("td,trd->tr", rows_block.astype(jnp.float32), down_picked).astype(jnp.bfloat16)
        up_picked = adapter_up[ids_block].astype(jnp.float32)
        return jnp.einsum("tr,trk->tk", low_rows.astype(jnp.float32), up_picked).astype(jnp.bfloat16)

    delta_rows = lax.map(block_delta, (token_blocks, id_blocks)).reshape(TOKENS, KV)
    return (base_sums + delta_rows.astype(jnp.float32)).astype(jnp.bfloat16)
```

```python
import functools

import jax
import jax.numpy as jnp
from jax import lax
from jax.experimental import pallas as pl
from jax.experimental.pallas import tpu as pltpu
from jax.sharding import PartitionSpec as P

MESH = pl.DeviceIdType.MESH
F32 = jnp.float32
BF16 = jnp.bfloat16


def kernel(
    n_tok,
    n_hid,
    pieces,
    rank,
    ids_ref,
    tokens_hbm,
    value_hbm,
    down_hbm,
    up_hbm,
    out_ref,
    tokens,
    value,
    adapters,
    core_send,
    core_recv,
    partial,
    chip_send,
    chip_recv,
    picked,
    wanted,
    low_send,
    low_recv,
    load_sem,
    right_sem,
    left_sem,
    line_sem,
    pair_send_sem,
    pair_recv_sem,
    core_send_sem,
    core_recv_sem,
    chip_send_sem,
    chip_recv_sem,
    low_send_sem,
    low_recv_sem,
):
    y = lax.axis_index("parts")
    z = lax.axis_index("tok")
    h = lax.axis_index("hid")
    chips = n_hid // 2
    core = lax.rem(h, 2)
    x = lax.div(h, 2)
    rows, depth = tokens.shape
    kv = out_ref.shape[1]
    lanes = adapters.shape[1]
    adp_dev = lanes // rank
    half = lanes // 2
    piece = half // pieces

    load_down = pltpu.make_async_copy(down_hbm, adapters.at[z, :, pl.ds(0, depth)], load_sem.at[0])
    load_up = pltpu.make_async_copy(up_hbm, adapters.at[z, :, pl.ds(depth, kv)], load_sem.at[1])
    load_tokens = pltpu.make_async_copy(tokens_hbm, tokens, load_sem.at[2])
    load_value = pltpu.make_async_copy(value_hbm, value, load_sem.at[3])
    load_down.start()
    load_up.start()
    load_tokens.start()
    load_value.start()

    barrier = pltpu.get_barrier_semaphore()
    pl.semaphore_signal(barrier, inc=1, device_id={"parts": 1 - y}, device_id_type=MESH)
    for d in range(1, n_hid):
        pl.semaphore_signal(
            barrier, inc=1, device_id={"hid": lax.rem(h + d, n_hid)}, device_id_type=MESH
        )

    @pl.when(z > 0)
    def _():
        pl.semaphore_signal(barrier, inc=1, device_id={"tok": z - 1}, device_id_type=MESH)

    @pl.when(z < n_tok - 1)
    def _():
        pl.semaphore_signal(barrier, inc=1, device_id={"tok": z + 1}, device_id_type=MESH)

    neighbours = (z > 0).astype(jnp.int32) + (z < n_tok - 1).astype(jnp.int32)
    pl.semaphore_wait(barrier, n_hid + neighbours)

    def chunk(block, side, c):
        start = pl.multiple_of(side * half + c * piece, piece)
        return adapters.at[block, pl.ds(start, piece)]

    def to_right(block, c):
        ref = chunk(block, y, c)
        return pltpu.make_async_remote_copy(
            src_ref=ref,
            dst_ref=ref,
            send_sem=right_sem.at[block, c],
            recv_sem=line_sem.at[block, c],
            device_id={"tok": z + 1},
            device_id_type=MESH,
        )

    def to_left(block, c):
        ref = chunk(block, y, c)
        return pltpu.make_async_remote_copy(
            src_ref=ref,
            dst_ref=ref,
            send_sem=left_sem.at[block, c],
            recv_sem=line_sem.at[block, c],
            device_id={"tok": z - 1},
            device_id_type=MESH,
        )

    def to_pair(block, side, c):
        ref = chunk(block, side, c)
        return pltpu.make_async_remote_copy(
            src_ref=ref,
            dst_ref=ref,
            send_sem=pair_send_sem.at[block, c],
            recv_sem=pair_recv_sem.at[block, c],
            device_id={"parts": 1 - y},
            device_id_type=MESH,
        )

    load_down.wait()
    load_up.wait()
    for c in range(pieces):
        @pl.when(z < n_tok - 1)
        def _():
            to_right(z, c).start()

        @pl.when(z > 0)
        def _():
            to_left(z, c).start()

    def forward(s):
        from_left = z - 1 - s
        from_right = z + 1 + s
        for c in range(pieces):
            @pl.when(from_left >= 0)
            def _():
                to_right(from_left, c).wait_recv()

                @pl.when(z < n_tok - 1)
                def _():
                    to_right(from_left, c).start()

                to_pair(from_left, y, c).start()

            @pl.when(from_right < n_tok)
            def _():
                to_left(from_right, c).wait_recv()

                @pl.when(z > 0)
                def _():
                    to_left(from_right, c).start()

                to_pair(from_right, y, c).start()

    load_tokens.wait()
    load_value.wait()

    def base_block(j):
        columns = pl.ds(pl.multiple_of(j * kv, kv), kv)
        return jnp.dot(tokens[...], value[:, columns], preferred_element_type=F32)

    def to_core(i):
        return pltpu.make_async_remote_copy(
            src_ref=core_send.at[i],
            dst_ref=core_recv.at[i],
            send_sem=core_send_sem.at[i],
            recv_sem=core_recv_sem.at[i],
            device_id={"hid": x * 2 + 1 - core},
            device_id_type=MESH,
        )

    def other_core(i, carry):
        core_send[i] = base_block(i * 2 + 1 - core).astype(BF16)
        to_core(i).start()
        return carry

    lax.fori_loop(0, chips, other_core, 0)

    def own_core(i, carry):
        partial[i] = base_block(i * 2 + core)
        return carry

    lax.fori_loop(0, chips, own_core, 0)

    forward(0)

    def to_chip(i, slot):
        return pltpu.make_async_remote_copy(
            src_ref=chip_send.at[i],
            dst_ref=chip_recv.at[slot],
            send_sem=chip_send_sem.at[i],
            recv_sem=chip_recv_sem.at[slot],
            device_id={"hid": i * 2 + core},
            device_id_type=MESH,
        )

    for d in range(1, chips):
        i = lax.rem(x + d, chips)
        to_core(i).wait_recv()
        chip_send[i] = (partial[i] + core_recv[i].astype(F32)).astype(BF16)
        to_chip(i, x).start()

    lane_adapter = lax.broadcasted_iota(jnp.int32, (rows, lanes), 1) // rank
    ids = jnp.transpose(jnp.broadcast_to(ids_ref[...], (lanes, rows)))
    wanted[...] = ids - lane_adapter

    def low_block(block):
        sums = lax.dot_general(
            tokens[...],
            adapters[block, :, 0:depth],
            (((1,), (1,)), ((), ())),
            preferred_element_type=F32,
        )
        return jnp.where(wanted[...] == block * adp_dev, sums, 0.0)

    picked[...] = low_block(z)

    def low_of(s):
        for sign in (-1, 1):
            block = z + sign * (1 + s)

            @pl.when((block >= 0) & (block < n_tok))
            def _():
                for c in range(pieces):
                    to_pair(block, 1 - y, c).wait_recv()
                picked[...] += low_block(block)

    def step(s, carry):
        forward(s + 1)
        low_of(s)
        return carry

    lax.fori_loop(0, n_tok - 2, step, 0)

    to_core(x).wait_recv()
    partial[x] += core_recv[x].astype(F32)
    for d in range(1, chips):
        i = lax.rem(x + d, chips)
        to_chip(i, i).wait_recv()
        partial[x] += chip_recv[i].astype(F32)

    low_of(n_tok - 2)

    fold = (
        lax.rem(lax.broadcasted_iota(jnp.int32, (rank, lanes), 1), rank)
        == lax.broadcasted_iota(jnp.int32, (rank, lanes), 0)
    ).astype(F32).astype(BF16)
    low_send[...] = lax.dot_general(
        fold,
        picked[...].astype(BF16),
        (((1,), (1,)), ((), ())),
        preferred_element_type=F32,
    ).astype(BF16)

    def to_hid(d, slot):
        return pltpu.make_async_remote_copy(
            src_ref=low_send,
            dst_ref=low_recv.at[slot],
            send_sem=low_send_sem.at[d],
            recv_sem=low_recv_sem.at[slot],
            device_id={"hid": lax.rem(h + d, n_hid)},
            device_id_type=MESH,
        )

    for d in range(1, n_hid):
        to_hid(d, h).start()
    low = low_send[...].astype(F32)
    for d in range(1, n_hid):
        slot = lax.rem(h + d, n_hid)
        to_hid(d, slot).wait_recv()
        low += low_recv[slot].astype(F32)
    low = low.astype(BF16)

    spread = lax.dot_general(low, fold, (((0,), (0,)), ((), ())), preferred_element_type=F32)
    group = 4 if n_tok % 4 == 0 else 1
    delta = None
    for g in range(0, n_tok, group):
        chosen = jnp.concatenate(
            [
                jnp.where(wanted[...] == b * adp_dev, spread, 0.0).astype(BF16)
                for b in range(g, g + group)
            ],
            axis=1,
        )
        weights = adapters[g : g + group, :, depth : depth + kv].reshape(group * lanes, kv)
        term = jnp.dot(chosen, weights, preferred_element_type=F32)
        delta = term if delta is None else delta + term
    out_ref[...] = (partial[x] + delta.astype(BF16).astype(F32)).astype(BF16)

    for d in range(1, n_hid):
        to_hid(d, h).wait_send()
    for i in range(chips):
        to_core(i).wait_send()
    for d in range(1, chips):
        to_chip(lax.rem(x + d, chips), x).wait_send()

    def drain(block, carry):
        for c in range(pieces):
            @pl.when((block <= z) & (z < n_tok - 1))
            def _():
                to_right(block, c).wait_send()

            @pl.when((block >= z) & (z > 0))
            def _():
                to_left(block, c).wait_send()

            @pl.when(block != z)
            def _():
                to_pair(block, y, c).wait_send()

        return carry

    lax.fori_loop(0, n_tok, drain, 0)


def per_device(n_tok, n_hid, tokens, adapter_ids, value_weight, adapter_down, adapter_up):
    rows, depth = tokens.shape
    adp_dev, rank, kv = adapter_up.shape
    lanes = adp_dev * rank
    chips = n_hid // 2
    pieces = 4 if n_tok <= 8 else 1
    vmem = pl.BlockSpec(memory_space=pltpu.VMEM)
    hbm = pl.BlockSpec(memory_space=pl.ANY)
    dma = pltpu.SemaphoreType.DMA
    return pl.pallas_call(
        functools.partial(kernel, n_tok, n_hid, pieces, rank),
        out_shape=jax.ShapeDtypeStruct((rows, kv), BF16),
        in_specs=[vmem, hbm, hbm, hbm, hbm],
        out_specs=vmem,
        scratch_shapes=[
            pltpu.VMEM((rows, depth), BF16),
            pltpu.VMEM(value_weight.shape, BF16),
            pltpu.VMEM((n_tok, lanes, depth + kv), BF16),
            pltpu.VMEM((chips, rows, kv), BF16),
            pltpu.VMEM((chips, rows, kv), BF16),
            pltpu.VMEM((chips, rows, kv), F32),
            pltpu.VMEM((chips, rows, kv), BF16),
            pltpu.VMEM((chips, rows, kv), BF16),
            pltpu.VMEM((rows, lanes), F32),
            pltpu.VMEM((rows, lanes), jnp.int32),
            pltpu.VMEM((rank, rows), BF16),
            pltpu.VMEM((n_hid, rank, rows), BF16),
            dma((4,)),
            dma((n_tok, pieces)),
            dma((n_tok, pieces)),
            dma((n_tok, pieces)),
            dma((n_tok, pieces)),
            dma((n_tok, pieces)),
            dma((chips,)),
            dma((chips,)),
            dma((chips,)),
            dma((chips,)),
            dma((n_hid,)),
            dma((n_hid,)),
        ],
        compiler_params=pltpu.CompilerParams(
            collective_id=0, has_side_effects=True, vmem_limit_bytes=60 * 1024 * 1024
        ),
    )(
        adapter_ids.reshape(1, rows),
        tokens,
        value_weight,
        adapter_down.reshape(lanes, depth),
        adapter_up.reshape(lanes, kv),
    )


def solution(mesh):
    in_specs = (
        P(("parts", "tok"), "hid"),
        P(("parts", "tok"), None),
        P("hid", None),
        P("tok", None, "hid"),
        P("tok", None, "hid"),
    )
    out_specs = P(("parts", "tok"), "hid")
    body = functools.partial(per_device, mesh.shape["tok"], mesh.shape["hid"])
    return jax.shard_map(body, mesh=mesh, in_specs=in_specs, out_specs=out_specs, check_vma=False)
```

```python
import functools

import jax
import jax.numpy as jnp
from jax import lax
from jax.experimental import pallas as pl
from jax.experimental.pallas import tpu as pltpu
from jax.sharding import PartitionSpec as P

MESH = pl.DeviceIdType.MESH
F32 = jnp.float32
BF16 = jnp.bfloat16


def kernel(
    n_tok,
    n_hid,
    pieces,
    rank,
    ids_ref,
    tokens_hbm,
    value_hbm,
    down_hbm,
    up_hbm,
    out_ref,
    tokens,
    value,
    adapters,
    core_send,
    core_recv,
    partial,
    chip_send,
    chip_recv,
    picked,
    wanted,
    low_send,
    low_recv,
    load_sem,
    right_sem,
    left_sem,
    line_sem,
    pair_send_sem,
    pair_recv_sem,
    core_send_sem,
    core_recv_sem,
    chip_send_sem,
    chip_recv_sem,
    low_send_sem,
    low_recv_sem,
):
    y = lax.axis_index("parts")
    z = lax.axis_index("tok")
    h = lax.axis_index("hid")
    chips = n_hid // 2
    core = lax.rem(h, 2)
    x = lax.div(h, 2)
    rows, depth = tokens.shape
    kv = out_ref.shape[1]
    lanes = adapters.shape[1]
    adp_dev = lanes // rank
    half = lanes // 2
    piece = half // pieces

    load_down = pltpu.make_async_copy(down_hbm, adapters.at[z, :, pl.ds(0, depth)], load_sem.at[0])
    load_up = pltpu.make_async_copy(up_hbm, adapters.at[z, :, pl.ds(depth, kv)], load_sem.at[1])
    load_tokens = pltpu.make_async_copy(tokens_hbm, tokens, load_sem.at[2])
    load_value = pltpu.make_async_copy(value_hbm, value, load_sem.at[3])
    load_down.start()
    load_up.start()
    load_tokens.start()
    load_value.start()

    barrier = pltpu.get_barrier_semaphore()
    pl.semaphore_signal(barrier, inc=1, device_id={"parts": 1 - y}, device_id_type=MESH)
    for d in range(1, n_hid):
        pl.semaphore_signal(
            barrier, inc=1, device_id={"hid": lax.rem(h + d, n_hid)}, device_id_type=MESH
        )

    @pl.when(z > 0)
    def _():
        pl.semaphore_signal(barrier, inc=1, device_id={"tok": z - 1}, device_id_type=MESH)

    @pl.when(z < n_tok - 1)
    def _():
        pl.semaphore_signal(barrier, inc=1, device_id={"tok": z + 1}, device_id_type=MESH)

    neighbours = (z > 0).astype(jnp.int32) + (z < n_tok - 1).astype(jnp.int32)
    pl.semaphore_wait(barrier, n_hid + neighbours)

    def chunk(block, side, c):
        start = pl.multiple_of(side * half + c * piece, piece)
        return adapters.at[block, pl.ds(start, piece)]

    def to_right(block, c):
        ref = chunk(block, y, c)
        return pltpu.make_async_remote_copy(
            src_ref=ref,
            dst_ref=ref,
            send_sem=right_sem.at[block, c],
            recv_sem=line_sem.at[block, c],
            device_id={"tok": z + 1},
            device_id_type=MESH,
        )

    def to_left(block, c):
        ref = chunk(block, y, c)
        return pltpu.make_async_remote_copy(
            src_ref=ref,
            dst_ref=ref,
            send_sem=left_sem.at[block, c],
            recv_sem=line_sem.at[block, c],
            device_id={"tok": z - 1},
            device_id_type=MESH,
        )

    def to_pair(block, side, c):
        ref = chunk(block, side, c)
        return pltpu.make_async_remote_copy(
            src_ref=ref,
            dst_ref=ref,
            send_sem=pair_send_sem.at[block, c],
            recv_sem=pair_recv_sem.at[block, c],
            device_id={"parts": 1 - y},
            device_id_type=MESH,
        )

    load_down.wait()
    load_up.wait()
    for c in range(pieces):
        @pl.when(z < n_tok - 1)
        def _():
            to_right(z, c).start()

        @pl.when(z > 0)
        def _():
            to_left(z, c).start()

    def forward(s, first, last):
        from_left = z - 1 - s
        from_right = z + 1 + s
        for c in range(first, last):
            @pl.when(from_left >= 0)
            def _():
                to_right(from_left, c).wait_recv()

                @pl.when(z < n_tok - 1)
                def _():
                    to_right(from_left, c).start()

                to_pair(from_left, y, c).start()

            @pl.when(from_right < n_tok)
            def _():
                to_left(from_right, c).wait_recv()

                @pl.when(z > 0)
                def _():
                    to_left(from_right, c).start()

                to_pair(from_right, y, c).start()

    load_tokens.wait()
    load_value.wait()

    def base_block(j):
        columns = pl.ds(pl.multiple_of(j * kv, kv), kv)
        return jnp.dot(tokens[...], value[:, columns], preferred_element_type=F32)

    def to_core(i):
        return pltpu.make_async_remote_copy(
            src_ref=core_send.at[i],
            dst_ref=core_recv.at[i],
            send_sem=core_send_sem.at[i],
            recv_sem=core_recv_sem.at[i],
            device_id={"hid": x * 2 + 1 - core},
            device_id_type=MESH,
        )

    passed = 0
    for k in range(2 * chips):
        i = k % chips
        if k < chips:
            core_send[i] = base_block(i * 2 + 1 - core).astype(BF16)
            to_core(i).start()
        else:
            partial[i] = base_block(i * 2 + core)
        upto = pieces * (k + 1) // (2 * chips)
        forward(0, passed, upto)
        passed = upto

    def to_chip(i, slot):
        return pltpu.make_async_remote_copy(
            src_ref=chip_send.at[i],
            dst_ref=chip_recv.at[slot],
            send_sem=chip_send_sem.at[i],
            recv_sem=chip_recv_sem.at[slot],
            device_id={"hid": i * 2 + core},
            device_id_type=MESH,
        )

    for d in range(1, chips):
        i = lax.rem(x + d, chips)
        to_core(i).wait_recv()
        chip_send[i] = (partial[i] + core_recv[i].astype(F32)).astype(BF16)
        to_chip(i, x).start()

    lane_adapter = lax.broadcasted_iota(jnp.int32, (rows, lanes), 1) // rank
    ids = jnp.transpose(jnp.broadcast_to(ids_ref[...], (lanes, rows)))
    wanted[...] = ids - lane_adapter

    def low_block(block):
        sums = lax.dot_general(
            tokens[...],
            adapters[block, :, 0:depth],
            (((1,), (1,)), ((), ())),
            preferred_element_type=F32,
        )
        return jnp.where(wanted[...] == block * adp_dev, sums, 0.0)

    picked[...] = low_block(z)

    def low_of(s):
        for sign in (-1, 1):
            block = z + sign * (1 + s)

            @pl.when((block >= 0) & (block < n_tok))
            def _():
                for c in range(pieces):
                    to_pair(block, 1 - y, c).wait_recv()
                picked[...] += low_block(block)

    def step(s, carry):
        forward(s + 1, 0, pieces)
        low_of(s)
        return carry

    lax.fori_loop(0, n_tok - 2, step, 0)

    to_core(x).wait_recv()
    partial[x] += core_recv[x].astype(F32)
    for d in range(1, chips):
        i = lax.rem(x + d, chips)
        to_chip(i, i).wait_recv()
        partial[x] += chip_recv[i].astype(F32)

    low_of(n_tok - 2)

    fold = (
        lax.rem(lax.broadcasted_iota(jnp.int32, (rank, lanes), 1), rank)
        == lax.broadcasted_iota(jnp.int32, (rank, lanes), 0)
    ).astype(F32).astype(BF16)
    low_send[...] = lax.dot_general(
        fold,
        picked[...].astype(BF16),
        (((1,), (1,)), ((), ())),
        preferred_element_type=F32,
    ).astype(BF16)

    def to_hid(d, slot):
        return pltpu.make_async_remote_copy(
            src_ref=low_send,
            dst_ref=low_recv.at[slot],
            send_sem=low_send_sem.at[d],
            recv_sem=low_recv_sem.at[slot],
            device_id={"hid": lax.rem(h + d, n_hid)},
            device_id_type=MESH,
        )

    for d in range(1, n_hid):
        to_hid(d, h).start()
    low = low_send[...].astype(F32)
    for d in range(1, n_hid):
        slot = lax.rem(h + d, n_hid)
        to_hid(d, slot).wait_recv()
        low += low_recv[slot].astype(F32)
    low = low.astype(BF16)

    spread = lax.dot_general(low, fold, (((0,), (0,)), ((), ())), preferred_element_type=F32)
    group = 4 if n_tok % 4 == 0 else 1
    delta = None
    for g in range(0, n_tok, group):
        chosen = jnp.concatenate(
            [
                jnp.where(wanted[...] == b * adp_dev, spread, 0.0).astype(BF16)
                for b in range(g, g + group)
            ],
            axis=1,
        )
        weights = adapters[g : g + group, :, depth : depth + kv].reshape(group * lanes, kv)
        term = jnp.dot(chosen, weights, preferred_element_type=F32)
        delta = term if delta is None else delta + term
    out_ref[...] = (partial[x] + delta.astype(BF16).astype(F32)).astype(BF16)

    for d in range(1, n_hid):
        to_hid(d, h).wait_send()
    for i in range(chips):
        to_core(i).wait_send()
    for d in range(1, chips):
        to_chip(lax.rem(x + d, chips), x).wait_send()

    def drain(block, carry):
        for c in range(pieces):
            @pl.when((block <= z) & (z < n_tok - 1))
            def _():
                to_right(block, c).wait_send()

            @pl.when((block >= z) & (z > 0))
            def _():
                to_left(block, c).wait_send()

            @pl.when(block != z)
            def _():
                to_pair(block, y, c).wait_send()

        return carry

    lax.fori_loop(0, n_tok, drain, 0)


def per_device(n_tok, n_hid, tokens, adapter_ids, value_weight, adapter_down, adapter_up):
    rows, depth = tokens.shape
    adp_dev, rank, kv = adapter_up.shape
    lanes = adp_dev * rank
    chips = n_hid // 2
    pieces = 8 if n_tok <= 8 else 1
    vmem = pl.BlockSpec(memory_space=pltpu.VMEM)
    hbm = pl.BlockSpec(memory_space=pltpu.HBM)
    dma = pltpu.SemaphoreType.DMA
    return pl.pallas_call(
        functools.partial(kernel, n_tok, n_hid, pieces, rank),
        out_shape=jax.ShapeDtypeStruct((rows, kv), BF16),
        in_specs=[vmem, hbm, hbm, hbm, hbm],
        out_specs=vmem,
        scratch_shapes=[
            pltpu.VMEM((rows, depth), BF16),
            pltpu.VMEM(value_weight.shape, BF16),
            pltpu.VMEM((n_tok, lanes, depth + kv), BF16),
            pltpu.VMEM((chips, rows, kv), BF16),
            pltpu.VMEM((chips, rows, kv), BF16),
            pltpu.VMEM((chips, rows, kv), F32),
            pltpu.VMEM((chips, rows, kv), BF16),
            pltpu.VMEM((chips, rows, kv), BF16),
            pltpu.VMEM((rows, lanes), F32),
            pltpu.VMEM((rows, lanes), jnp.int32),
            pltpu.VMEM((rank, rows), BF16),
            pltpu.VMEM((n_hid, rank, rows), BF16),
            dma((4,)),
            dma((n_tok, pieces)),
            dma((n_tok, pieces)),
            dma((n_tok, pieces)),
            dma((n_tok, pieces)),
            dma((n_tok, pieces)),
            dma((chips,)),
            dma((chips,)),
            dma((chips,)),
            dma((chips,)),
            dma((n_hid,)),
            dma((n_hid,)),
        ],
        compiler_params=pltpu.CompilerParams(
            collective_id=0, has_side_effects=True, vmem_limit_bytes=60 * 1024 * 1024
        ),
    )(
        adapter_ids.reshape(1, rows),
        tokens,
        value_weight,
        adapter_down.reshape(lanes, depth),
        adapter_up.reshape(lanes, kv),
    )


def solution(mesh):
    in_specs = (
        P(("parts", "tok"), "hid"),
        P(("parts", "tok"), None),
        P("hid", None),
        P("tok", None, "hid"),
        P("tok", None, "hid"),
    )
    out_specs = P(("parts", "tok"), "hid")
    body = functools.partial(per_device, mesh.shape["tok"], mesh.shape["hid"])
    return jax.shard_map(body, mesh=mesh, in_specs=in_specs, out_specs=out_specs, check_vma=False)
```

```python
import functools

import jax
import jax.numpy as jnp
from jax import lax
from jax.experimental import pallas as pl
from jax.experimental.pallas import tpu as pltpu
from jax.sharding import PartitionSpec as P

MESH = pl.DeviceIdType.MESH
F32 = jnp.float32
BF16 = jnp.bfloat16


def kernel(
    n_tok,
    n_hid,
    pieces,
    extra,
    rank,
    ids_ref,
    tokens_hbm,
    value_hbm,
    down_hbm,
    up_hbm,
    out_ref,
    tokens,
    value,
    adapters,
    core_send,
    core_recv,
    partial,
    chip_send,
    chip_recv,
    picked,
    wanted,
    low_send,
    low_recv,
    load_sem,
    right_sem,
    left_sem,
    line_sem,
    pair_send_sem,
    pair_recv_sem,
    core_send_sem,
    core_recv_sem,
    chip_send_sem,
    chip_recv_sem,
    low_send_sem,
    low_recv_sem,
):
    y = lax.axis_index("parts")
    z = lax.axis_index("tok")
    h = lax.axis_index("hid")
    chips = n_hid // 2
    core = lax.rem(h, 2)
    x = lax.div(h, 2)
    rows, depth = tokens.shape
    kv = out_ref.shape[1]
    lanes = adapters.shape[1]
    adp_dev = lanes // rank
    half = lanes // 2
    piece = half // pieces

    load_down = pltpu.make_async_copy(down_hbm, adapters.at[z, :, pl.ds(0, depth)], load_sem.at[0])
    load_up = pltpu.make_async_copy(up_hbm, adapters.at[z, :, pl.ds(depth, kv)], load_sem.at[1])
    load_tokens = pltpu.make_async_copy(tokens_hbm, tokens, load_sem.at[2])
    load_value = pltpu.make_async_copy(value_hbm, value, load_sem.at[3])
    load_down.start()
    load_up.start()

    barrier = pltpu.get_barrier_semaphore()
    pl.semaphore_signal(barrier, inc=1, device_id={"parts": 1 - y}, device_id_type=MESH)
    for d in range(1, n_hid):
        pl.semaphore_signal(
            barrier, inc=1, device_id={"hid": lax.rem(h + d, n_hid)}, device_id_type=MESH
        )

    @pl.when(z > 0)
    def _():
        pl.semaphore_signal(barrier, inc=1, device_id={"tok": z - 1}, device_id_type=MESH)

    @pl.when(z < n_tok - 1)
    def _():
        pl.semaphore_signal(barrier, inc=1, device_id={"tok": z + 1}, device_id_type=MESH)

    load_down.wait()
    load_up.wait()
    load_tokens.start()
    load_value.start()

    neighbours = (z > 0).astype(jnp.int32) + (z < n_tok - 1).astype(jnp.int32)
    pl.semaphore_wait(barrier, n_hid + neighbours)

    def chunk(block, side, c):
        start = pl.multiple_of(side * half + c * piece, piece)
        return adapters.at[block, pl.ds(start, piece)]

    def line_chunk(block, c):
        return chunk(block, y, c) if c < pieces else chunk(block, 1 - y, c - extra)

    def to_right(block, c):
        ref = line_chunk(block, c)
        return pltpu.make_async_remote_copy(
            src_ref=ref,
            dst_ref=ref,
            send_sem=right_sem.at[block, c],
            recv_sem=line_sem.at[block, c],
            device_id={"tok": z + 1},
            device_id_type=MESH,
        )

    def to_left(block, c):
        ref = line_chunk(block, c)
        return pltpu.make_async_remote_copy(
            src_ref=ref,
            dst_ref=ref,
            send_sem=left_sem.at[block, c],
            recv_sem=line_sem.at[block, c],
            device_id={"tok": z - 1},
            device_id_type=MESH,
        )

    def to_pair(block, side, c):
        ref = chunk(block, side, c)
        return pltpu.make_async_remote_copy(
            src_ref=ref,
            dst_ref=ref,
            send_sem=pair_send_sem.at[block, c],
            recv_sem=pair_recv_sem.at[block, c],
            device_id={"parts": 1 - y},
            device_id_type=MESH,
        )

    for c in range(pieces):
        @pl.when(z < n_tok - 1)
        def _():
            to_right(z, c).start()

        @pl.when(z > 0)
        def _():
            to_left(z, c).start()

    for c in range(pieces, pieces + extra):
        @pl.when(z == 0)
        def _():
            to_right(z, c).start()

        @pl.when(z == n_tok - 1)
        def _():
            to_left(z, c).start()

    def by_pair(block, c):
        return c < pieces - extra or (block != 0) & (block != n_tok - 1)

    def forward(s, first, last):
        from_left = z - 1 - s
        from_right = z + 1 + s
        for c in range(first, last):
            @pl.when(from_left >= 0 if c < pieces else from_left == 0)
            def _():
                to_right(from_left, c).wait_recv()

                @pl.when(z < n_tok - 1)
                def _():
                    to_right(from_left, c).start()

                if c < pieces:
                    @pl.when(by_pair(from_left, c))
                    def _():
                        to_pair(from_left, y, c).start()

            @pl.when(from_right < n_tok if c < pieces else from_right == n_tok - 1)
            def _():
                to_left(from_right, c).wait_recv()

                @pl.when(z > 0)
                def _():
                    to_left(from_right, c).start()

                if c < pieces:
                    @pl.when(by_pair(from_right, c))
                    def _():
                        to_pair(from_right, y, c).start()

    load_tokens.wait()
    load_value.wait()

    def base_block(j):
        columns = pl.ds(pl.multiple_of(j * kv, kv), kv)
        return jnp.dot(tokens[...], value[:, columns], preferred_element_type=F32)

    def to_core(i):
        return pltpu.make_async_remote_copy(
            src_ref=core_send.at[i],
            dst_ref=core_recv.at[i],
            send_sem=core_send_sem.at[i],
            recv_sem=core_recv_sem.at[i],
            device_id={"hid": x * 2 + 1 - core},
            device_id_type=MESH,
        )

    passed = 0
    for k in range(2 * chips):
        i = k % chips
        if k < chips:
            core_send[i] = base_block(i * 2 + 1 - core).astype(BF16)
            to_core(i).start()
        else:
            partial[i] = base_block(i * 2 + core)
        upto = pieces * (k + 1) // (2 * chips)
        forward(0, passed, upto)
        passed = upto

    forward(0, pieces, pieces + extra)

    def to_chip(i, slot):
        return pltpu.make_async_remote_copy(
            src_ref=chip_send.at[i],
            dst_ref=chip_recv.at[slot],
            send_sem=chip_send_sem.at[i],
            recv_sem=chip_recv_sem.at[slot],
            device_id={"hid": i * 2 + core},
            device_id_type=MESH,
        )

    for d in range(1, chips):
        i = lax.rem(x + d, chips)
        to_core(i).wait_recv()
        chip_send[i] = (partial[i] + core_recv[i].astype(F32)).astype(BF16)
        to_chip(i, x).start()

    lane_adapter = lax.broadcasted_iota(jnp.int32, (rows, lanes), 1) // rank
    ids = jnp.transpose(jnp.broadcast_to(ids_ref[...], (lanes, rows)))
    wanted[...] = ids - lane_adapter

    def low_block(block):
        sums = lax.dot_general(
            tokens[...],
            adapters[block, :, 0:depth],
            (((1,), (1,)), ((), ())),
            preferred_element_type=F32,
        )
        return jnp.where(wanted[...] == block * adp_dev, sums, 0.0)

    picked[...] = low_block(z)

    def low_of(s):
        for sign in (-1, 1):
            block = z + sign * (1 + s)

            @pl.when((block >= 0) & (block < n_tok))
            def _():
                for c in range(pieces):
                    @pl.when(by_pair(block, c))
                    def _():
                        to_pair(block, 1 - y, c).wait_recv()

                picked[...] += low_block(block)

    def step(s, carry):
        forward(s + 1, 0, pieces + extra)
        low_of(s)
        return carry

    lax.fori_loop(0, n_tok - 2, step, 0)

    to_core(x).wait_recv()
    partial[x] += core_recv[x].astype(F32)
    for d in range(1, chips):
        i = lax.rem(x + d, chips)
        to_chip(i, i).wait_recv()
        partial[x] += chip_recv[i].astype(F32)

    low_of(n_tok - 2)

    fold = (
        lax.rem(lax.broadcasted_iota(jnp.int32, (rank, lanes), 1), rank)
        == lax.broadcasted_iota(jnp.int32, (rank, lanes), 0)
    ).astype(F32).astype(BF16)
    low_send[...] = lax.dot_general(
        fold,
        picked[...].astype(BF16),
        (((1,), (1,)), ((), ())),
        preferred_element_type=F32,
    ).astype(BF16)

    def to_hid(d, slot):
        return pltpu.make_async_remote_copy(
            src_ref=low_send,
            dst_ref=low_recv.at[slot],
            send_sem=low_send_sem.at[d],
            recv_sem=low_recv_sem.at[slot],
            device_id={"hid": lax.rem(h + d, n_hid)},
            device_id_type=MESH,
        )

    for d in range(1, n_hid):
        to_hid(d, h).start()
    low = low_send[...].astype(F32)
    for d in range(1, n_hid):
        slot = lax.rem(h + d, n_hid)
        to_hid(d, slot).wait_recv()
        low += low_recv[slot].astype(F32)
    low = low.astype(BF16)

    spread = lax.dot_general(low, fold, (((0,), (0,)), ((), ())), preferred_element_type=F32)
    group = 4 if n_tok % 4 == 0 else 1
    delta = None
    for g in range(0, n_tok, group):
        chosen = jnp.concatenate(
            [
                jnp.where(wanted[...] == b * adp_dev, spread, 0.0).astype(BF16)
                for b in range(g, g + group)
            ],
            axis=1,
        )
        weights = adapters[g : g + group, :, depth : depth + kv].reshape(group * lanes, kv)
        term = jnp.dot(chosen, weights, preferred_element_type=F32)
        delta = term if delta is None else delta + term
    out_ref[...] = (partial[x] + delta.astype(BF16).astype(F32)).astype(BF16)

    for d in range(1, n_hid):
        to_hid(d, h).wait_send()
    for i in range(chips):
        to_core(i).wait_send()
    for d in range(1, chips):
        to_chip(lax.rem(x + d, chips), x).wait_send()

    def drain(block, carry):
        for c in range(pieces + extra):
            @pl.when((block <= z if c < pieces else block == 0) & (z < n_tok - 1))
            def _():
                to_right(block, c).wait_send()

            @pl.when((block >= z if c < pieces else block == n_tok - 1) & (z > 0))
            def _():
                to_left(block, c).wait_send()

            if c < pieces:
                @pl.when((block != z) & by_pair(block, c))
                def _():
                    to_pair(block, y, c).wait_send()

        return carry

    lax.fori_loop(0, n_tok, drain, 0)


def per_device(n_tok, n_hid, tokens, adapter_ids, value_weight, adapter_down, adapter_up):
    rows, depth = tokens.shape
    adp_dev, rank, kv = adapter_up.shape
    lanes = adp_dev * rank
    chips = n_hid // 2
    pieces = 8 if n_tok <= 8 else 1
    extra = 2 if pieces == 8 else 0
    vmem = pl.BlockSpec(memory_space=pltpu.VMEM)
    hbm = pl.BlockSpec(memory_space=pltpu.HBM)
    dma = pltpu.SemaphoreType.DMA
    return pl.pallas_call(
        functools.partial(kernel, n_tok, n_hid, pieces, extra, rank),
        out_shape=jax.ShapeDtypeStruct((rows, kv), BF16),
        in_specs=[vmem, hbm, hbm, hbm, hbm],
        out_specs=vmem,
        scratch_shapes=[
            pltpu.VMEM((rows, depth), BF16),
            pltpu.VMEM(value_weight.shape, BF16),
            pltpu.VMEM((n_tok, lanes, depth + kv), BF16),
            pltpu.VMEM((chips, rows, kv), BF16),
            pltpu.VMEM((chips, rows, kv), BF16),
            pltpu.VMEM((chips, rows, kv), F32),
            pltpu.VMEM((chips, rows, kv), BF16),
            pltpu.VMEM((chips, rows, kv), BF16),
            pltpu.VMEM((rows, lanes), F32),
            pltpu.VMEM((rows, lanes), jnp.int32),
            pltpu.VMEM((rank, rows), BF16),
            pltpu.VMEM((n_hid, rank, rows), BF16),
            dma((4,)),
            dma((n_tok, pieces + extra)),
            dma((n_tok, pieces + extra)),
            dma((n_tok, pieces + extra)),
            dma((n_tok, pieces)),
            dma((n_tok, pieces)),
            dma((chips,)),
            dma((chips,)),
            dma((chips,)),
            dma((chips,)),
            dma((n_hid,)),
            dma((n_hid,)),
        ],
        compiler_params=pltpu.CompilerParams(
            collective_id=0, has_side_effects=True, vmem_limit_bytes=60 * 1024 * 1024
        ),
    )(
        adapter_ids.reshape(1, rows),
        tokens,
        value_weight,
        adapter_down.reshape(lanes, depth),
        adapter_up.reshape(lanes, kv),
    )


def solution(mesh):
    in_specs = (
        P(("parts", "tok"), "hid"),
        P(("parts", "tok"), None),
        P("hid", None),
        P("tok", None, "hid"),
        P("tok", None, "hid"),
    )
    out_specs = P(("parts", "tok"), "hid")
    body = functools.partial(per_device, mesh.shape["tok"], mesh.shape["hid"])
    return jax.shard_map(body, mesh=mesh, in_specs=in_specs, out_specs=out_specs, check_vma=False)
```
